256 devices in a mesh: dp: 4 (over x), ep: 64 (over y, z, core).
Axes of the slice: x: 4, y: 4, z: 8, core: 2. Of those that a mesh axis runs over, the one named last changes fastest.
Arguments:
- tokens: bfloat16 [2048, 3584], P(('dp', 'ep')), may hold values from -6 to 6
- expert_ids: int32 [2, 2048, 8], P(None, ('dp', 'ep')), may hold values from 0 to 63, all different within a row; in each aligned block of 8 rows (0 to 7, 8 to 15, ..., all dimensions but the last counted through in order) at most 2 rows name the same one
- quant_gates: int32 [2, 2048, 8], P(None, ('dp', 'ep')), may hold values from 1 to 63
- w_gate: bfloat16 [2, 64, 3584, 1024], P(None, 'ep', None, 'dp'), may hold values from -0.09375 to 0.09375
- w_up: bfloat16 [2, 64, 3584, 1024], P(None, 'ep', None, 'dp'), may hold values from -0.09375 to 0.09375
- w_down: bfloat16 [2, 64, 1024, 3584], P(None, 'ep', 'dp'), may hold values from -0.1875 to 0.1875
Outputs:
- stream_out: bfloat16 [2048, 3584], P(('dp', 'ep'))
- expert_load: int32 [2, 64], replicated
The draws below stay inside these ranges and needn't reach their ends.
Inputs may be any that keep to these rules, and one draw needn't show every extreme that they name: `expert_ids`: in each layer, the 8 tokens of one device name any one expert at most 2 times, a bound that some block reaches.
All inputs are finite; a program needn't handle non-finite values.
Results may differ from the reference program's by a relative error of at most 0.015.
Values may be sent and summed in bfloat16 or wider, within the bound.
No kernel may reach another device: no remote copies, remote signals or barrier semaphores. Data moves between devices by JAX's collectives and lax.ppermute only.
A program may use at most 64 MiB of HBM per device.

```python
import math
import jax
import jax.numpy as jnp
import numpy as np
from jax import lax

D = 3584
FFW = 1024
TOP = 8
LAYERS = 2
TOK_DEV = 8
EXPERTS = 64
CAP = 2
FF_DEV = 256
TOKENS = 2048
N_DP = 4
N_EP = 64


def place_ends(values, rng, low, largest):
    place = [jax.random.randint(jax.random.fold_in(rng, axis), (), 0, length) for axis, length in enumerate(values.shape)]
    widest = values.shape.index(max(values.shape))
    neighbour = place[:widest] + [(place[widest] + 1) % values.shape[widest]] + place[widest + 1:]
    return values.at[tuple(place)].set(low).at[tuple(neighbour)].set(largest)


def block_scale(own_key, dims, pieces, low, largest):
    gain = 1.0
    for dim, blocks in pieces:
        draws = jax.random.uniform(jax.random.fold_in(jax.random.fold_in(own_key, 6), dim), (blocks,), jnp.float32, low / len(pieces), largest / len(pieces))
        gain = gain * jnp.repeat(jnp.exp(draws), dims[dim] // blocks).reshape((-1,) + (1,) * (len(dims) - 1 - dim))
    return gain


def shared_out(own_key, own, number, rows, number_of, top, limit, slope):
    sequence = jax.random.permutation(own_key, number_of)
    packed, ordinary = load_shares(number_of, rows * top, limit, slope, True), load_shares(number_of, rows * top, limit, slope, False)
    places = jnp.arange(number_of)

    def named(lengths, rotation):
        used = int((lengths > 0).sum())
        fixed = max(1, used // 4)
        moved = fixed + (places - fixed + rotation * (used - fixed)) % max(1, number_of - fixed)
        return jnp.zeros((number_of,), jnp.int32).at[sequence[jnp.where(places < fixed, places, moved)]].set(jnp.asarray(lengths, jnp.int32))

    lengths = jnp.where(number % 4 == 0, named(packed, number // 4), named(ordinary, number - number // 4 - 1))
    mixed = jax.random.permutation(jax.random.fold_in(own, 3), number_of)
    donor, taker = mixed[0:number_of // 2 * 2:2], mixed[1:number_of // 2 * 2:2]
    room = jnp.minimum(lengths[donor] - 1, limit - lengths[taker]) // 2
    room = jnp.where((donor == sequence[0]) | (taker == sequence[0]) | (lengths[taker] == 0), 0, jnp.maximum(room, 0))
    moved = jax.random.randint(jax.random.fold_in(own, 4), (number_of // 2,), 0, 1 << 20) % (room + 1)
    lengths = lengths.at[donor].add(-moved).at[taker].add(moved)
    members = jnp.searchsorted(jnp.cumsum(lengths), jnp.arange(rows * top), side="right").astype(jnp.int32)
    table = members.reshape(top, rows).T
    table = table[jax.random.permutation(jax.random.fold_in(own, 1), rows)]
    rotation = jax.random.randint(jax.random.fold_in(own, 2), (rows, 1), 0, top)
    return jnp.take_along_axis(table, (jnp.arange(top)[None, :] + rotation) % top, axis=1)


def load_shares(number_of, total, reach, lean, full):
    weights = [(1 << 20) // math.isqrt(standing ** lean) + 1 for standing in range(1, number_of + 1)]
    largest = reach if full else min(reach, max(-(-total // number_of), total * weights[0] // sum(weights)))
    least = 1 if total - largest >= number_of - 1 else 0
    given, spare = [largest] + [least] * (number_of - 1), total - largest - least * (number_of - 1)
    while spare > 0:
        free = [i for i in range(1, number_of) if given[i] < largest] or [i for i in range(1, number_of) if given[i] < reach]
        whole, budget = sum([weights[i] for i in free]), spare
        for i in free:
            extra = min(reach - given[i], max(1, budget * weights[i] // whole), spare)
            given[i] = given[i] + extra
            spare = spare - extra
    return np.array(given)


def bell_draw(stream_key, extent, scale, most, shards=(), dtype=jnp.bfloat16):
    factor_of = block_scale(stream_key, extent, shards, -0.22, 0.18) if shards else 1.0
    drawn = jax.random.normal(stream_key, extent, jnp.float32) * scale * factor_of
    return jnp.minimum(jnp.maximum(drawn, -most), most).astype(dtype)


def setup_inputs(seed: int = 0) -> dict:
    key_list = jax.random.split(jax.random.key(seed), 7)
    tokens = bell_draw(key_list[0], (TOKENS, D), 1.0, 6.0, ((0, 256),))
    expert_ids_keys = jax.random.split(jax.random.fold_in(key_list[1], 1), LAYERS * TOKENS // TOK_DEV)
    expert_ids_turns = jax.random.permutation(jax.random.fold_in(key_list[1], 3), LAYERS * TOKENS // TOK_DEV)
    expert_ids = jax.vmap(lambda own, number: shared_out(jax.random.fold_in(key_list[1], 2), own, number, TOK_DEV, EXPERTS, TOP, CAP, 2))(expert_ids_keys, expert_ids_turns).reshape((LAYERS, TOKENS, TOP))
    quant_gates = place_ends(jax.random.randint(key_list[2], (LAYERS, TOKENS, TOP), 1, 64), jax.random.fold_in(key_list[2], 1), 1, 63).astype(jnp.int32)
    w_gate = bell_draw(key_list[3], (LAYERS, EXPERTS, D, FFW), D ** -0.5, 0.09375, ((1, 64), (3, 4)))
    w_up = bell_draw(key_list[4], (LAYERS, EXPERTS, D, FFW), D ** -0.5, 0.09375, ((1, 64), (3, 4)))
    w_down = bell_draw(key_list[5], (LAYERS, EXPERTS, FFW, D), FFW ** -0.5, 0.1875, ((1, 64), (2, 4)))
    return dict(tokens=tokens, expert_ids=expert_ids, quant_gates=quant_gates, w_gate=w_gate, w_up=w_up, w_down=w_down)


ROUTE_SCALE = 2.827
EPS = 1e-06

def expert_rows(rows, weight_gate, weight_up, weight_down):
    gate = jnp.dot(rows, weight_gate, preferred_element_type=jnp.float32)
    upper = jnp.dot(rows, weight_up, preferred_element_type=jnp.float32)
    hidden = (jax.nn.silu(gate) * upper).astype(jnp.bfloat16)
    total = jnp.zeros((rows.shape[0], D), jnp.float32)
    for block in range(N_DP):
        lower_edge = block * FF_DEV
        piece = jnp.dot(hidden[:, lower_edge:lower_edge + FF_DEV], weight_down[lower_edge:lower_edge + FF_DEV], preferred_element_type=jnp.float32)
        total = total + piece.astype(jnp.bfloat16).astype(jnp.float32)
    return total

def reference(tokens, expert_ids, quant_gates, w_gate, w_up, w_down):
    state = tokens
    most_rows = CAP * N_DP * N_EP
    loads = []
    for layer in range(LAYERS):
        wide = state.astype(jnp.float32)
        normed = (wide * lax.rsqrt(lax.optimization_barrier(jnp.mean(wide * wide, axis=1, keepdims=True)) + EPS)).astype(jnp.bfloat16)
        flat_ids = expert_ids[layer].reshape(TOKENS * TOP).astype(jnp.int32)
        quant = quant_gates[layer].astype(jnp.float32)
        gates = (ROUTE_SCALE * quant / lax.optimization_barrier(jnp.sum(quant, axis=1, keepdims=True))).reshape(TOKENS * TOP)
        expert_iota = lax.broadcasted_iota(jnp.int32, (1, EXPERTS), 1)
        loads.append(lax.optimization_barrier(jnp.sum((flat_ids[:, None] == expert_iota).astype(jnp.int32), axis=0)).astype(jnp.int32))

        def one_expert(expert, accum):
            order = jnp.argsort((flat_ids != expert).astype(jnp.int32), stable=True)[:most_rows].astype(jnp.int32)
            valid = flat_ids[order] == expert
            token_index = (order // TOP).astype(jnp.int32)
            rows = normed[token_index]
            result = expert_rows(rows, w_gate[layer, expert], w_up[layer, expert], w_down[layer, expert])
            weight = jnp.where(valid, gates[order], jnp.float32(0.0))
            return accum.at[token_index].add(weight[:, None] * result)
        branch = lax.fori_loop(0, EXPERTS, one_expert, jnp.zeros((TOKENS, D), jnp.float32))
        state = (state.astype(jnp.float32) + branch).astype(jnp.bfloat16)
    return (state, jnp.stack(loads))
```

```python
import jax
import jax.numpy as jnp
from jax import lax
from jax.sharding import Mesh
from jax.sharding import PartitionSpec as P

EP = ("ep_0", "ep_1", "ep_2")
DP_EP = ("dp", "ep_0", "ep_1", "ep_2")

ROUTE_SCALE = 2.827
EPS = 1e-06
BF16 = jnp.bfloat16
F32 = jnp.float32


def shift(array, step):
    n_dp = lax.axis_size("dp")
    return lax.ppermute(array, "dp", [(i, (i + step) % n_dp) for i in range(n_dp)])


def ring_gather(own, dim):
    half = own.shape[dim] // 2
    left = shift(own, 1)
    right = shift(own, -1)
    first = shift(lax.slice_in_dim(left, 0, half, axis=dim), 1)
    second = shift(lax.slice_in_dim(right, half, 2 * half, axis=dim), -1)
    return own, left, right, lax.concatenate([first, second], dim)


def to_column_slices(weight):
    n_dp = lax.axis_size("dp")
    me = lax.axis_index("dp")
    width = weight.shape[1] // n_dp

    def columns_of(step):
        return lax.dynamic_slice_in_dim(weight, ((me + step) % n_dp) * width, width, axis=1)

    return columns_of(0), shift(columns_of(1), 1), shift(columns_of(-1), -1), shift(columns_of(2), 2)


def dot(a, b):
    return jnp.dot(a, b, preferred_element_type=F32)


def slot_picks(ids, experts, capacity, lines):
    rows, top = ids.shape
    tokens = rows // lines
    expert_iota = lax.broadcasted_iota(jnp.int32, (lines, tokens * top, experts), 2)
    onehot = (ids.reshape(lines, tokens * top)[:, :, None] == expert_iota).astype(F32)
    before = jnp.tril(jnp.ones((tokens * top, tokens * top), F32), -1)
    earlier = jnp.einsum("ab,lbe->lae", before, onehot, preferred_element_type=F32)
    place = jnp.sum(earlier * onehot, axis=2).astype(jnp.int32).reshape(rows, top)
    line = lax.broadcasted_iota(jnp.int32, (rows, top), 0) // tokens
    target = (ids * lines + line) * capacity + place
    slot_iota = lax.broadcasted_iota(jnp.int32, (rows, top, experts * lines * capacity), 2)
    return target[:, :, None] == slot_iota


def gates_of(quant):
    wide = quant.astype(F32)
    return ROUTE_SCALE * wide / jnp.sum(wide, axis=1, keepdims=True)


def swap(rows):
    return lax.all_to_all(rows, EP, split_axis=0, concat_axis=0, tiled=True)


def per_device(tokens, expert_ids, quant_gates, w_gate, w_up, w_down):
    layers, count_tok, top = expert_ids.shape
    n_dp = lax.axis_size("dp")
    n_ep = lax.axis_size(EP)
    me = lax.axis_index("dp")
    capacity = min(count_tok, max(2, 3 * count_tok * top // (2 * n_ep)))
    width = tokens.shape[1]
    part = width // n_dp

    expert_iota = lax.broadcasted_iota(jnp.int32, (1, 1, n_ep), 2)
    counts = jnp.sum(
        (expert_ids.reshape(layers, count_tok * top)[:, :, None] == expert_iota).astype(jnp.int32), axis=1
    )
    loads = counts
    for axis in DP_EP:
        loads = lax.psum(loads, axis)

    routes = lax.all_gather(jnp.stack([expert_ids, quant_gates]), "dp", axis=2, tiled=True)
    line_ids, line_quant = routes[0], routes[1]
    state = lax.all_to_all(tokens, "dp", split_axis=1, concat_axis=0, tiled=True)

    for layer in range(layers):
        weight_gate = w_gate[layer, 0]
        weight_up = w_up[layer, 0]
        slices = to_column_slices(w_down[layer, 0])
        picked = slot_picks(line_ids[layer], n_ep, capacity, n_dp)
        spread = jnp.sum(jnp.where(picked, gates_of(line_quant[layer])[:, :, None], 0.0), axis=1)
        if layer == 0:
            wide = tokens.astype(F32)
            normed = (wide * lax.rsqrt(jnp.mean(wide * wide, axis=1, keepdims=True) + EPS)).astype(BF16)
            own = jnp.any(slot_picks(expert_ids[0], n_ep, capacity, 1), axis=1).astype(BF16)
            arrived = swap(dot(own.T, normed).astype(BF16))
            hidden = []
            for block in ring_gather(arrived, 1):
                hidden.append((jax.nn.silu(dot(block, weight_gate)) * dot(block, weight_up)).astype(BF16))
            hidden = jnp.concatenate(hidden, axis=0)
            count = n_ep * n_dp * capacity
            out_row = lax.broadcasted_iota(jnp.int32, (count, count), 0)
            in_row = lax.broadcasted_iota(jnp.int32, (count, count), 1)
            ring = in_row // (n_ep * capacity)
            away = jnp.where(ring == 0, 0, jnp.where(ring == 1, n_dp - 1, jnp.where(ring == 2, 1, 2)))
            in_slot = in_row % (n_ep * capacity)
            moved = ((in_slot // capacity) * n_dp + (me + away) % n_dp) * capacity + in_slot % capacity
            hidden = dot((out_row == moved).astype(BF16), hidden).astype(BF16)
        else:
            chosen = jnp.any(picked, axis=1).astype(BF16)
            arrived = swap(dot(chosen.T, state).astype(BF16))
            gate, upper, square = 0.0, 0.0, 0.0
            for step, block in zip((0, -1, 1, 2), ring_gather(arrived, 0)):
                start = ((me + step) % n_dp) * part
                gate = gate + dot(block, lax.dynamic_slice_in_dim(weight_gate, start, part, axis=0))
                upper = upper + dot(block, lax.dynamic_slice_in_dim(weight_up, start, part, axis=0))
                wide = block.astype(F32)
                square = square + jnp.sum(wide * wide, axis=1, keepdims=True)
            scale = lax.rsqrt(square / width + EPS)
            hidden = (jax.nn.silu(gate * scale) * (upper * scale)).astype(BF16)
        result = 0.0
        for block, weight in zip(ring_gather(hidden, 0), slices):
            result = result + dot(block, weight)
        returned = swap(result.astype(BF16))
        branch = jnp.dot(
            spread, returned.astype(F32), precision=lax.Precision.HIGHEST, preferred_element_type=F32
        )
        state = (state.astype(F32) + branch).astype(BF16)
    stream = lax.all_to_all(state, "dp", split_axis=0, concat_axis=1, tiled=True)
    return (stream, loads)


def solution(mesh):
    finer = Mesh(mesh.devices.reshape(mesh.shape["dp"], 4, 8, 2), DP_EP)
    placed = (
        P(DP_EP, None),
        P(None, DP_EP, None),
        P(None, DP_EP, None),
        P(None, EP, None, "dp"),
        P(None, EP, None, "dp"),
        P(None, EP, "dp", None),
    )
    return jax.shard_map(
        per_device, mesh=finer, in_specs=placed, out_specs=(P(DP_EP, None), P()), check_vma=False
    )
```

```python
import functools

import jax
import jax.numpy as jnp
from jax import lax
from jax.experimental import pallas as pl
from jax.experimental.pallas import tpu as pltpu
from jax.sharding import Mesh
from jax.sharding import PartitionSpec as P


EP = ("ep_0", "ep_1", "ep_2")
DP_EP = ("dp", "ep_0", "ep_1", "ep_2")

ROUTE_SCALE = 2.827
EPS = 1e-06
BF16 = jnp.bfloat16
F32 = jnp.float32
LANES = 128
STEPS = (0, -1, 1, 2)


def shift(array, step):
    n_dp = lax.axis_size("dp")
    return lax.ppermute(array, "dp", [(i, (i + step) % n_dp) for i in range(n_dp)])


def ring_gather(own, dim):
    half = own.shape[dim] // 2
    left, right = shift(own, 1), shift(own, -1)
    first = shift(lax.slice_in_dim(left, 0, half, axis=dim), 1)
    second = shift(lax.slice_in_dim(right, half, 2 * half, axis=dim), -1)
    return own, left, right, first, second


def exchange(piece_for):
    got = []
    for step in STEPS:
        got.append(shift(piece_for(-step), -step) if step else piece_for(0))
    return got


def place_blocks(blocks, dim):
    n_dp = lax.axis_size("dp")
    shape = list(blocks[0].shape)
    length = shape[dim]
    shape[dim] *= n_dp
    out = jnp.zeros(shape, blocks[0].dtype)
    for step, block in zip(STEPS, blocks):
        start = ((lax.axis_index("dp") + step) % n_dp) * length
        out = lax.dynamic_update_slice_in_dim(out, block, start, axis=dim)
    return out


def dot(a, b):
    return jnp.dot(a, b, preferred_element_type=F32)


def silu_times(gate, upper):
    return gate / (1.0 + jnp.exp(-gate)) * upper


def vmem(count):
    return [pl.BlockSpec(memory_space=pltpu.VMEM)] * count


def down_kernel(*refs):
    count = len(STEPS)
    hidden, weights, out_ref = refs[:count], refs[count : 2 * count], refs[2 * count]
    total = dot(hidden[0][...], weights[0][...])
    for hidden_ref, weight_ref in zip(hidden[1:], weights[1:]):
        total = total + dot(hidden_ref[...], weight_ref[...])
    out_ref[...] = total.astype(out_ref.dtype)


def down(hidden, weights):
    rows, units = hidden[0].shape
    part = weights[0].shape[1]
    return pl.pallas_call(
        down_kernel,
        out_shape=jax.ShapeDtypeStruct((rows, part), BF16),
        in_specs=vmem(2 * len(hidden)),
        out_specs=vmem(1)[0],
        cost_estimate=pl.CostEstimate(
            flops=2 * rows * units * part * len(hidden), bytes_accessed=2 * units * part * len(hidden), transcendentals=0
        ),
        name="down",
    )(*hidden, *weights)


def two_parts(value):
    high = value.astype(BF16)
    low = (value - high.astype(F32)).astype(BF16)
    lane = lax.broadcasted_iota(jnp.int32, (value.shape[0], LANES), 1)
    wide = jnp.where(lane == 0, high.astype(F32), jnp.where(lane == 1, low.astype(F32), 0.0))
    return wide.astype(BF16)


def one_value(parts):
    return jnp.sum(parts.astype(F32), axis=1, keepdims=True)


def partial_kernel(me_ref, rows_ref, order_ref, *refs):
    n_dp = len(STEPS)
    gates, ups, outs = refs[:n_dp], refs[n_dp : 2 * n_dp], refs[2 * n_dp :]
    height = outs[0].shape[0]
    units = gates[0].shape[1]
    for plane, out_ref in enumerate(outs):
        rows = dot(order_ref[plane * height : (plane + 1) * height, :], rows_ref[...]).astype(BF16)
        for step, gate_ref, up_ref in zip(STEPS, gates, ups):
            at = pl.multiple_of(((me_ref[0] + step + n_dp) % n_dp) * 2 * units, 2 * units)
            out_ref[:, pl.ds(at, units)] = dot(rows, gate_ref[...]).astype(BF16)
            out_ref[:, pl.ds(at + units, units)] = dot(rows, up_ref[...]).astype(BF16)
        wide = rows.astype(F32)
        out_ref[:, 2 * n_dp * units :] = two_parts(jnp.sum(wide * wide, axis=1, keepdims=True))


def partial_products(me, rows, order, gates, ups):
    count, part = rows.shape
    n_dp = len(STEPS)
    units = gates[0].shape[1]
    width = 2 * n_dp * units + LANES
    return pl.pallas_call(
        partial_kernel,
        out_shape=[jax.ShapeDtypeStruct((count // n_dp, width), BF16)] * n_dp,
        in_specs=[pl.BlockSpec(memory_space=pltpu.SMEM)] + vmem(2 + 2 * n_dp),
        out_specs=vmem(n_dp),
        cost_estimate=pl.CostEstimate(
            flops=2 * count * part * (2 * n_dp * units + count), bytes_accessed=4 * n_dp * part * units, transcendentals=0
        ),
        name="partial_products",
    )(me, rows, order, *gates, *ups)


def fold_kernel(left_ref, right_ref, from_left_ref, from_right_ref, left_out, right_out):
    half = from_left_ref.shape[1]
    last = left_ref.shape[1] - LANES
    right_out[:, :half] = (right_ref[:, :half].astype(F32) + from_left_ref[...].astype(F32)).astype(BF16)
    right_out[:, half:] = right_ref[:, half:]
    left_out[:, :half] = left_ref[:, :half]
    left_out[:, half:last] = (
        left_ref[:, half:last].astype(F32) + from_right_ref[:, : last - half].astype(F32)
    ).astype(BF16)
    left_out[:, last:] = two_parts(one_value(left_ref[:, last:]) + one_value(from_right_ref[:, last - half :]))


def fold(left, right, from_left, from_right):
    return pl.pallas_call(
        fold_kernel,
        out_shape=[jax.ShapeDtypeStruct(left.shape, BF16)] * 2,
        in_specs=vmem(4),
        out_specs=vmem(2),
        cost_estimate=pl.CostEstimate(flops=left.size * 8, bytes_accessed=left.size * 8, transcendentals=0),
        name="fold",
    )(left, right, from_left, from_right)


def finish_kernel(width, me_ref, own_ref, left_ref, right_ref, note_ref, w0, w1, w2, w3, w4, out_ref, hidden_ref):
    n_dp = len(STEPS)
    units = w1.shape[0]
    last = own_ref.shape[1] - LANES

    def total(start, size):
        at = slice(start, start + size)
        return own_ref[:, at].astype(F32) + left_ref[:, at].astype(F32) + right_ref[:, at].astype(F32)

    square = one_value(own_ref[:, last:]) + one_value(left_ref[:, last:]) + one_value(right_ref[:, last:])
    scale = lax.rsqrt(square / width + EPS)
    for i in range(n_dp):
        gate = total(2 * i * units, units) * scale
        upper = total((2 * i + 1) * units, units) * scale
        hidden_ref[:, i * units : (i + 1) * units] = silu_times(gate, upper).astype(BF16)

    def block(step):
        at = pl.multiple_of(((me_ref[0] + step + n_dp) % n_dp) * units, units)
        return hidden_ref[:, pl.ds(at, units)]

    opposite = block(STEPS[3])
    half = units // 2
    result = dot(block(STEPS[0]), w0[0, 0]) + dot(block(STEPS[1]), w1[...])
    result = result + dot(block(STEPS[2]), w2[...])
    result = result + dot(opposite[:, :half], w3[...]) + dot(opposite[:, half:], w4[...])
    out_ref[:, :width] = result.astype(BF16)
    out_ref[:, width:] = jnp.broadcast_to(note_ref[...], (out_ref.shape[0], LANES))


def finish(me, own, left, right, note, w_down, layer, others):
    rows = own.shape[0]
    _, _, units, width = w_down.shape
    n_dp = len(STEPS)
    return pl.pallas_call(
        functools.partial(finish_kernel, width),
        out_shape=jax.ShapeDtypeStruct((rows, width + LANES), BF16),
        grid=(1,),
        in_specs=[pl.BlockSpec(memory_space=pltpu.SMEM)]
        + vmem(4)
        + [pl.BlockSpec((1, 1, units, width), lambda i: (layer, 0, 0, 0))]
        + vmem(len(others)),
        out_specs=vmem(1)[0],
        scratch_shapes=[pltpu.VMEM((rows, n_dp * units), BF16)],
        cost_estimate=pl.CostEstimate(
            flops=2 * rows * n_dp * units * width, bytes_accessed=2 * n_dp * units * width, transcendentals=rows * n_dp * units
        ),
        name="finish",
    )(me, own, left, right, note, w_down, *others)


def slot_picks(ids, experts, capacity, lines):
    rows, top = ids.shape
    tokens = rows // lines
    expert_iota = lax.broadcasted_iota(jnp.int32, (lines, tokens * top, experts), 2)
    onehot = (ids.reshape(lines, tokens * top)[:, :, None] == expert_iota).astype(F32)
    before = jnp.tril(jnp.ones((tokens * top, tokens * top), F32), -1)
    earlier = jnp.einsum("ab,lbe->lae", before, onehot, preferred_element_type=F32)
    place = jnp.sum(earlier * onehot, axis=2).astype(jnp.int32).reshape(rows, top)
    line = lax.broadcasted_iota(jnp.int32, (rows, top), 0) // tokens
    target = (ids * lines + line) * capacity + place
    slot_iota = lax.broadcasted_iota(jnp.int32, (rows, top, experts * lines * capacity), 2)
    return target[:, :, None] == slot_iota


def gates_of(quant):
    wide = quant.astype(F32)
    return ROUTE_SCALE * wide / jnp.sum(wide, axis=1, keepdims=True)


def spread_of(picked, quant):
    return jnp.sum(jnp.where(picked, gates_of(quant)[:, :, None], 0.0), axis=1)


def chosen_of(picked):
    return jnp.any(picked, axis=1).astype(BF16)


def swap(rows):
    return lax.all_to_all(rows, EP, split_axis=0, concat_axis=0, tiled=True)


def weighted(spread, rows):
    return jnp.dot(spread, rows.astype(F32), precision=lax.Precision.HIGHEST, preferred_element_type=F32)


def per_device(tokens, expert_ids, quant_gates, w_gate, w_up, w_down):
    layers, count_tok, top = expert_ids.shape
    n_dp = lax.axis_size("dp")
    n_ep = lax.axis_size(EP)
    me = lax.axis_index("dp").astype(jnp.int32)
    me_vector = me.reshape(1)
    capacity = min(count_tok, max(2, 3 * count_tok * top // (2 * n_ep)))
    width = tokens.shape[1]
    units = w_gate.shape[3]
    part = width // n_dp
    slots = n_ep * capacity
    count = n_dp * slots

    def around(step, size):
        return ((me + step) % n_dp) * size

    wide = tokens.astype(F32)
    normed = (wide * lax.rsqrt(jnp.mean(wide * wide, axis=1, keepdims=True) + EPS)).astype(BF16)
    own_picks = [slot_picks(expert_ids[i], n_ep, capacity, 1) for i in range(layers)]
    arrived = swap(dot(chosen_of(own_picks[0]).T, normed).astype(BF16))

    down_slices = exchange(
        lambda step: lax.dynamic_slice(w_down, (0, 0, 0, around(step, part)), (1, 1, units, part))[0, 0]
    )
    routes = jnp.concatenate([*expert_ids, *quant_gates], axis=1).astype(BF16)
    routes = jnp.pad(routes, ((0, 0), (0, LANES - routes.shape[1])))
    line = exchange(
        lambda step: jnp.concatenate(
            [lax.dynamic_slice_in_dim(tokens, around(step, part), part, axis=1), routes], axis=1
        ),
    )
    line = place_blocks(line, 0)
    state = line[:, :part]
    routes = line[:, part:].astype(jnp.int32)
    line_ids = [routes[:, i * top : (i + 1) * top] for i in range(layers)]
    line_quant = [routes[:, (layers + i) * top : (layers + i + 1) * top] for i in range(layers)]
    line_picks = [slot_picks(ids, n_ep, capacity, n_dp) for ids in line_ids]
    expert_iota = lax.broadcasted_iota(jnp.int32, (1, 1, n_ep), 2)
    counts = jnp.concatenate(
        [jnp.sum((ids[:, :, None] == expert_iota).astype(F32), axis=(0, 1)) for ids in line_ids]
    )
    note = jnp.pad(counts, (0, LANES - layers * n_ep)).astype(BF16).reshape(1, LANES)

    def rows_of(weight):
        return lambda step: lax.dynamic_slice(weight, (1, 0, around(step, part), 0), (1, 1, part, units))[0, 0]

    gates = exchange(rows_of(w_gate))
    ups = exchange(rows_of(w_up))
    whole_down = ring_gather(w_down[1, 0], 0)[1:]

    own, left, right, first, second = ring_gather(arrived, 1)
    hidden = []
    for block in (own, left, right, jnp.concatenate([first, second], axis=1)):
        hidden.append(silu_times(dot(block, w_gate[0, 0]), dot(block, w_up[0, 0])).astype(BF16))
    hidden = jnp.concatenate(hidden, axis=0)
    out_row = lax.broadcasted_iota(jnp.int32, (count, count), 0)
    in_row = lax.broadcasted_iota(jnp.int32, (count, count), 1)

    def moved(row):
        place = row // slots
        away = jnp.where(place == 0, 0, jnp.where(place == 1, n_dp - 1, jnp.where(place == 2, 1, 2)))
        slot = row % slots
        return ((slot // capacity) * n_dp + (me + away) % n_dp) * capacity + slot % capacity

    hidden = dot((out_row == moved(in_row)).astype(BF16), hidden).astype(BF16)
    order = (moved(out_row) == in_row).astype(BF16)
    blocks = exchange(lambda step: hidden)
    returned = swap(down(blocks, down_slices))
    branch = weighted(spread_of(line_picks[0], line_quant[0]), returned)
    state = (state.astype(F32) + branch).astype(BF16)

    arrived = swap(dot(chosen_of(line_picks[1]).T, state).astype(BF16))
    own_rows = exchange(lambda step: lax.dynamic_slice_in_dim(state, around(step, count_tok), count_tok, axis=0))
    own_rows = place_blocks(own_rows, 1)
    own, left, right, opposite = partial_products(me_vector, arrived, order, gates, ups)
    half = n_dp * units
    from_left, from_right = shift(opposite[:, :half], 1), shift(opposite[:, half:], -1)
    left, right = fold(left, right, from_left, from_right)
    from_left, from_right = shift(right, 1), shift(left, -1)
    message = finish(me_vector, own, from_left, from_right, note, w_down, 1, whole_down)
    returned = swap(message)
    branch = weighted(spread_of(own_picks[1], quant_gates[1]), returned[:, :width])
    stream_out = (own_rows.astype(F32) + branch).astype(BF16)
    total = jnp.sum(returned[:, width:].astype(F32).reshape(n_ep, capacity, LANES)[:, 0], axis=0)
    loads = total[: layers * n_ep].astype(jnp.int32).reshape(layers, n_ep)
    return (stream_out, loads)


def solution(mesh):
    finer = Mesh(mesh.devices.reshape(mesh.shape["dp"], 4, 8, 2), DP_EP)
    placed = (
        P(DP_EP, None),
        P(None, DP_EP, None),
        P(None, DP_EP, None),
        P(None, EP, None, "dp"),
        P(None, EP, None, "dp"),
        P(None, EP, "dp", None),
    )

    return jax.shard_map(per_device, mesh=finer, in_specs=placed, out_specs=(P(DP_EP, None), P()), check_vma=False)
```

```python
import functools

import jax
import jax.numpy as jnp
from jax import lax
from jax.experimental import pallas as pl
from jax.experimental.pallas import tpu as pltpu
from jax.sharding import Mesh
from jax.sharding import PartitionSpec as P


EP = ("ep_0", "ep_1", "ep_2")
DP_EP = ("dp", "ep_0", "ep_1", "ep_2")

ROUTE_SCALE = 2.827
EPS = 1e-06
BF16 = jnp.bfloat16
F32 = jnp.float32
LANES = 128
CHUNK = 512
ROWS = 256
GRANT = 20 * 1024 * 1024
STEPS = (0, -1, 1, 2)


def shift(array, step):
    n_dp = lax.axis_size("dp")
    return lax.ppermute(array, "dp", [(i, (i + step) % n_dp) for i in range(n_dp)])


def ring_gather(own, dim):
    half = own.shape[dim] // 2
    left, right = shift(own, 1), shift(own, -1)
    first = shift(lax.slice_in_dim(left, 0, half, axis=dim), 1)
    second = shift(lax.slice_in_dim(right, half, 2 * half, axis=dim), -1)
    return own, left, right, first, second


def exchange(piece_for):
    got = []
    for step in STEPS:
        got.append(shift(piece_for(-step), -step) if step else piece_for(0))
    return got


def place_blocks(blocks, dim):
    n_dp = lax.axis_size("dp")
    shape = list(blocks[0].shape)
    length = shape[dim]
    shape[dim] *= n_dp
    out = jnp.zeros(shape, blocks[0].dtype)
    for step, block in zip(STEPS, blocks):
        start = ((lax.axis_index("dp") + step) % n_dp) * length
        out = lax.dynamic_update_slice_in_dim(out, block, start, axis=dim)
    return out


def dot(a, b):
    return jnp.dot(a, b, preferred_element_type=F32)


def silu_times(gate, upper):
    return gate / (1.0 + jnp.exp(-gate)) * upper


def vmem(count):
    return [pl.BlockSpec(memory_space=pltpu.VMEM)] * count


def loop(count):
    return pl.loop(0, count)


def rows_at(index, size):
    return pl.ds(pl.multiple_of(index * size, size), size)


def hbm(count):
    return [pl.BlockSpec(memory_space=pltpu.HBM)] * count


def down_kernel(*refs):
    count = len(STEPS)
    hidden, weights, out_ref = refs[:count], refs[count : 2 * count], refs[2 * count]

    @loop(out_ref.shape[0] // ROWS)
    def _(i):
        at = rows_at(i, ROWS)
        total = dot(hidden[0][at, :], weights[0][...])
        for hidden_ref, weight_ref in zip(hidden[1:], weights[1:]):
            total = total + dot(hidden_ref[at, :], weight_ref[...])
        out_ref[at, :] = total.astype(out_ref.dtype)


def down(hidden, weights):
    rows, units = hidden[0].shape
    part = weights[0].shape[1]
    return pl.pallas_call(
        down_kernel,
        out_shape=jax.ShapeDtypeStruct((rows, part), BF16),
        in_specs=vmem(2 * len(hidden)),
        out_specs=vmem(1)[0],
        cost_estimate=pl.CostEstimate(
            flops=2 * rows * units * part * len(hidden), bytes_accessed=2 * units * part * len(hidden), transcendentals=0
        ),
        compiler_params=pltpu.CompilerParams(vmem_limit_bytes=GRANT),
        name="down",
    )(*hidden, *weights)


def two_parts(value):
    high = value.astype(BF16)
    low = (value - high.astype(F32)).astype(BF16)
    lane = lax.broadcasted_iota(jnp.int32, (value.shape[0], LANES), 1)
    wide = jnp.where(lane == 0, high.astype(F32), jnp.where(lane == 1, low.astype(F32), 0.0))
    return wide.astype(BF16)


def one_value(parts):
    return jnp.sum(parts.astype(F32), axis=1, keepdims=True)


def spread_place(row, me, slots, capacity):
    n_dp = len(STEPS)
    place = row // slots
    away = jnp.where(place == 0, 0, jnp.where(place == 1, n_dp - 1, jnp.where(place == 2, 1, 2)))
    slot = row % slots
    return ((slot // capacity) * n_dp + (me + away) % n_dp) * capacity + slot % capacity


def partial_kernel(capacity, starts_ref, rows_ref, *refs):
    sources, (out_ref, arrived, sorted_ref, held, done) = refs[:-5], refs[-5:]
    count, _, units = held.shape
    total = sorted_ref.shape[0]
    first = pltpu.make_async_copy(rows_ref, arrived, done.at[count])
    copies = [pltpu.make_async_copy(source, held.at[k], done.at[k]) for k, source in enumerate(sources)]
    first.start()
    for copy in copies:
        copy.start()
    first.wait()

    @loop(total // ROWS)
    def _(i):
        at = rows_at(i, ROWS)
        row = lax.broadcasted_iota(jnp.int32, (ROWS, total), 0) + i * ROWS
        wanted = spread_place(row, starts_ref[count], total // len(STEPS), capacity)
        order = (wanted == lax.broadcasted_iota(jnp.int32, (ROWS, total), 1)).astype(F32).astype(BF16)
        rows = dot(order, arrived[...])
        sorted_ref[at, :] = rows.astype(BF16)
        out_ref[at, count * units :] = two_parts(jnp.sum(rows * rows, axis=1, keepdims=True))

    for copy in copies:
        copy.wait()

    @loop(count)
    def _(k):
        start = pl.multiple_of(starts_ref[k], units)
        out_ref[:, pl.ds(start, units)] = dot(sorted_ref[...], held[k]).astype(BF16)


def partial_products(me, rows, capacity, gates, ups):
    count, part = rows.shape
    n_dp = len(STEPS)
    units = gates[0].shape[1]
    weights = [weight for pair in zip(gates, ups) for weight in pair]
    starts = jnp.stack([(2 * ((me + step) % n_dp) + k) * units for step in STEPS for k in range(2)] + [me])
    return pl.pallas_call(
        functools.partial(partial_kernel, capacity),
        out_shape=jax.ShapeDtypeStruct((count, len(weights) * units + LANES), BF16),
        in_specs=[pl.BlockSpec(memory_space=pltpu.SMEM)] + hbm(1 + len(weights)),
        out_specs=vmem(1)[0],
        scratch_shapes=[
            pltpu.VMEM((count, part), BF16),
            pltpu.VMEM((count, part), BF16),
            pltpu.VMEM((len(weights), part, units), BF16),
            pltpu.SemaphoreType.DMA((len(weights) + 1,)),
        ],
        cost_estimate=pl.CostEstimate(
            flops=2 * count * part * (len(weights) * units + count), bytes_accessed=4 * n_dp * part * units, transcendentals=0
        ),
        compiler_params=pltpu.CompilerParams(vmem_limit_bytes=GRANT),
        name="partial_products",
    )(starts, rows, *weights)


def fold_kernel(left_ref, right_ref, from_left_ref, from_right_ref, left_out, right_out):
    half = from_left_ref.shape[0]
    last = left_ref.shape[1] - LANES
    for ref, arrived, out, at, other in (
        (right_ref, from_left_ref, right_out, slice(0, half), slice(half, 2 * half)),
        (left_ref, from_right_ref, left_out, slice(half, 2 * half), slice(0, half)),
    ):
        out[other, :] = ref[other, :]
        out[at, :last] = (ref[at, :last].astype(F32) + arrived[:, :last].astype(F32)).astype(BF16)
        out[at, last:] = two_parts(one_value(ref[at, last:]) + one_value(arrived[:, last:]))


def fold(products, from_left, from_right):
    height, width = products.shape[0] // len(STEPS), products.shape[1]
    return pl.pallas_call(
        fold_kernel,
        out_shape=[jax.ShapeDtypeStruct((height, width), BF16)] * 2,
        grid=(1,),
        in_specs=[pl.BlockSpec((height, width), lambda i: (1, 0)), pl.BlockSpec((height, width), lambda i: (2, 0))] + vmem(2),
        out_specs=vmem(2),
        cost_estimate=pl.CostEstimate(flops=height * width * 8, bytes_accessed=height * width * 8, transcendentals=0),
        compiler_params=pltpu.CompilerParams(vmem_limit_bytes=GRANT),
        name="fold",
    )(products, products, from_left, from_right)


def finish_kernel(layer, me_ref, products, left_ref, right_ref, w0, w1, w2, w3, w4, out_ref, hidden_ref, own_ref, held, done):
    n_dp = len(STEPS)
    units = w1.shape[0]
    half = units // 2
    width = out_ref.shape[1]
    last = own_ref.shape[1] - LANES
    first = pltpu.make_async_copy(products.at[: own_ref.shape[0]], own_ref, done.at[5])
    first.start()
    targets = [held.at[i] for i in range(3)] + [held.at[3, :half], held.at[3, half:]]
    copies = [
        pltpu.make_async_copy(source, target, done.at[k])
        for k, (source, target) in enumerate(zip((w0.at[layer, 0], w1, w2, w3, w4), targets))
    ]
    for copy in copies:
        copy.start()
    first.wait()

    def total(start, size):
        at = slice(start, start + size)
        return own_ref[:, at].astype(F32) + left_ref[:, at].astype(F32) + right_ref[:, at].astype(F32)

    square = one_value(own_ref[:, last:]) + one_value(left_ref[:, last:]) + one_value(right_ref[:, last:])
    scale = lax.rsqrt(square / width + EPS)
    for i in range(n_dp):
        gate = total(2 * i * units, units) * scale
        upper = total((2 * i + 1) * units, units) * scale
        hidden_ref[:, i * units : (i + 1) * units] = silu_times(gate, upper).astype(BF16)
    for copy in copies:
        copy.wait()

    def block(step):
        at = pl.multiple_of(((me_ref[0] + step + n_dp) % n_dp) * units, units)
        return hidden_ref[:, pl.ds(at, units)]

    @loop(width // CHUNK)
    def _(i):
        at = rows_at(i, CHUNK)
        result = dot(block(STEPS[0]), held[0, :, at])
        for k in range(1, n_dp):
            result = result + dot(block(STEPS[k]), held[k, :, at])
        out_ref[:, at] = result.astype(BF16)


def finish(me, products, left, right, w_down, layer, others):
    rows = left.shape[0]
    _, _, units, width = w_down.shape
    n_dp = len(STEPS)
    return pl.pallas_call(
        functools.partial(finish_kernel, layer),
        out_shape=jax.ShapeDtypeStruct((rows, width), BF16),
        in_specs=[pl.BlockSpec(memory_space=pltpu.SMEM)] + hbm(1) + vmem(2) + hbm(1 + len(others)),
        out_specs=vmem(1)[0],
        scratch_shapes=[
            pltpu.VMEM((rows, n_dp * units), BF16),
            pltpu.VMEM(left.shape, BF16),
            pltpu.VMEM((n_dp, units, width), BF16),
            pltpu.SemaphoreType.DMA((2 + len(others),)),
        ],
        cost_estimate=pl.CostEstimate(
            flops=2 * rows * n_dp * units * width, bytes_accessed=2 * n_dp * units * width, transcendentals=rows * n_dp * units
        ),
        compiler_params=pltpu.CompilerParams(vmem_limit_bytes=GRANT),
        name="finish",
    )(me, products, left, right, w_down, *others)


def slot_picks(ids, experts, capacity, lines):
    rows, top = ids.shape
    tokens = rows // lines
    expert_iota = lax.broadcasted_iota(jnp.int32, (lines, tokens * top, experts), 2)
    onehot = (ids.reshape(lines, tokens * top)[:, :, None] == expert_iota).astype(F32)
    before = jnp.tril(jnp.ones((tokens * top, tokens * top), F32), -1)
    earlier = jnp.einsum("ab,lbe->lae", before, onehot, preferred_element_type=F32)
    place = jnp.sum(earlier * onehot, axis=2).astype(jnp.int32).reshape(rows, top)
    line = lax.broadcasted_iota(jnp.int32, (rows, top), 0) // tokens
    target = (ids * lines + line) * capacity + place
    slot_iota = lax.broadcasted_iota(jnp.int32, (rows, top, experts * lines * capacity), 2)
    return target[:, :, None] == slot_iota


def gates_of(quant):
    wide = quant.astype(F32)
    return ROUTE_SCALE * wide / jnp.sum(wide, axis=1, keepdims=True)


def spread_of(picked, quant):
    return jnp.sum(jnp.where(picked, gates_of(quant)[:, :, None], 0.0), axis=1)


def chosen_of(picked):
    return jnp.any(picked, axis=1).astype(BF16)


def swap(rows):
    return lax.all_to_all(rows, EP, split_axis=0, concat_axis=0, tiled=True)


def weighted(spread, rows):
    return jnp.dot(spread, rows.astype(F32), precision=lax.Precision.HIGHEST, preferred_element_type=F32)


def per_device(tokens, expert_ids, quant_gates, w_gate, w_up, w_down):
    layers, count_tok, top = expert_ids.shape
    n_dp = lax.axis_size("dp")
    n_ep = lax.axis_size(EP)
    me = lax.axis_index("dp").astype(jnp.int32)
    me_vector = me.reshape(1)
    capacity = min(count_tok, max(2, 3 * count_tok * top // (2 * n_ep)))
    width = tokens.shape[1]
    units = w_gate.shape[3]
    part = width // n_dp
    slots = n_ep * capacity
    count = n_dp * slots

    def around(step, size):
        return ((me + step) % n_dp) * size

    wide = tokens.astype(F32)
    normed = (wide * lax.rsqrt(jnp.mean(wide * wide, axis=1, keepdims=True) + EPS)).astype(BF16)
    own_picks = [slot_picks(expert_ids[i], n_ep, capacity, 1) for i in range(layers)]
    arrived = swap(dot(chosen_of(own_picks[0]).T, normed).astype(BF16))

    down_slices = exchange(
        lambda step: lax.dynamic_slice(w_down, (0, 0, 0, around(step, part)), (1, 1, units, part))[0, 0]
    )
    routes = jnp.concatenate([*expert_ids, *quant_gates], axis=1).astype(BF16)
    routes = jnp.pad(routes, ((0, 0), (0, LANES - routes.shape[1])))
    line = exchange(
        lambda step: jnp.concatenate(
            [lax.dynamic_slice_in_dim(tokens, around(step, part), part, axis=1), routes], axis=1
        ),
    )
    line = place_blocks(line, 0)
    state = line[:, :part]
    routes = line[:, part:].astype(jnp.int32)
    line_ids = [routes[:, i * top : (i + 1) * top] for i in range(layers)]
    line_quant = [routes[:, (layers + i) * top : (layers + i + 1) * top] for i in range(layers)]
    line_picks = [slot_picks(ids, n_ep, capacity, n_dp) for ids in line_ids]
    expert_iota = lax.broadcasted_iota(jnp.int32, (1, 1, n_ep), 2)
    loads = jnp.stack([jnp.sum((ids[:, :, None] == expert_iota).astype(jnp.int32), axis=(0, 1)) for ids in line_ids])
    for axis in EP:
        loads = lax.psum(loads, axis)

    def rows_of(weight):
        return lambda step: lax.dynamic_slice(weight, (1, 0, around(step, part), 0), (1, 1, part, units))[0, 0]

    gates = exchange(rows_of(w_gate))
    ups = exchange(rows_of(w_up))
    whole_down = ring_gather(w_down[1, 0], 0)[1:]

    own, left, right, first, second = ring_gather(arrived, 1)
    hidden = []
    for block in (own, left, right, jnp.concatenate([first, second], axis=1)):
        hidden.append(silu_times(dot(block, w_gate[0, 0]), dot(block, w_up[0, 0])).astype(BF16))
    hidden = jnp.concatenate(hidden, axis=0)
    out_row = lax.broadcasted_iota(jnp.int32, (count, count), 0)
    in_row = lax.broadcasted_iota(jnp.int32, (count, count), 1)
    moved = out_row == spread_place(in_row, me, slots, capacity)
    hidden = dot(moved.astype(BF16), hidden).astype(BF16)
    blocks = exchange(lambda step: hidden)
    returned = swap(down(blocks, down_slices))
    branch = weighted(spread_of(line_picks[0], line_quant[0]), returned)
    state = (state.astype(F32) + branch).astype(BF16)

    arrived = swap(dot(chosen_of(line_picks[1]).T, state).astype(BF16))
    own_rows = exchange(lambda step: lax.dynamic_slice_in_dim(state, around(step, count_tok), count_tok, axis=0))
    own_rows = place_blocks(own_rows, 1)
    products = partial_products(me, arrived, capacity, gates, ups)
    middle = count - slots // 2
    from_left, from_right = shift(products[count - slots : middle], 1), shift(products[middle:], -1)
    left, right = fold(products, from_left, from_right)
    from_left, from_right = shift(right, 1), shift(left, -1)
    message = finish(me_vector, products, from_left, from_right, w_down, 1, whole_down)
    returned = swap(message)
    branch = weighted(spread_of(own_picks[1], quant_gates[1]), returned)
    stream_out = (own_rows.astype(F32) + branch).astype(BF16)
    return (stream_out, loads)


def solution(mesh):
    finer = Mesh(mesh.devices.reshape(mesh.shape["dp"], 4, 8, 2), DP_EP)
    placed = (
        P(DP_EP, None),
        P(None, DP_EP, None),
        P(None, DP_EP, None),
        P(None, EP, None, "dp"),
        P(None, EP, None, "dp"),
        P(None, EP, "dp", None),
    )

    return jax.shard_map(per_device, mesh=finer, in_specs=placed, out_specs=(P(DP_EP, None), P()), check_vma=False)
```

```python
import functools

import jax
import jax.numpy as jnp
from jax import lax
from jax.experimental import pallas as pl
from jax.experimental.pallas import tpu as pltpu
from jax.sharding import Mesh
from jax.sharding import PartitionSpec as P


EP = ("ep_0", "ep_1", "ep_2")
DP_EP = ("dp", "ep_0", "ep_1", "ep_2")

ROUTE_SCALE = 2.827
EPS = 1e-06
BF16 = jnp.bfloat16
F32 = jnp.float32
LANES = 128
CHUNK = 512
ROWS = 256
GRANT = 20 * 1024 * 1024
STEPS = (0, -1, 1, 2)


def shift(array, step):
    n_dp = lax.axis_size("dp")
    return lax.ppermute(array, "dp", [(i, (i + step) % n_dp) for i in range(n_dp)])


def ring_gather(own, dim):
    half = own.shape[dim] // 2
    left, right = shift(own, 1), shift(own, -1)
    first = shift(lax.slice_in_dim(left, 0, half, axis=dim), 1)
    second = shift(lax.slice_in_dim(right, half, 2 * half, axis=dim), -1)
    return own, left, right, first, second


def exchange(piece_for):
    got = []
    for step in STEPS:
        got.append(shift(piece_for(-step), -step) if step else piece_for(0))
    return got


def place_blocks(blocks, dim):
    n_dp = lax.axis_size("dp")
    shape = list(blocks[0].shape)
    length = shape[dim]
    shape[dim] *= n_dp
    out = jnp.zeros(shape, blocks[0].dtype)
    for step, block in zip(STEPS, blocks):
        start = ((lax.axis_index("dp") + step) % n_dp) * length
        out = lax.dynamic_update_slice_in_dim(out, block, start, axis=dim)
    return out


def dot(a, b):
    return jnp.dot(a, b, preferred_element_type=F32)


def silu_times(gate, upper):
    return gate / (1.0 + jnp.exp(-gate)) * upper


def vmem(count):
    return [pl.BlockSpec(memory_space=pltpu.VMEM)] * count


def loop(count):
    return pl.loop(0, count)


def rows_at(index, size):
    return pl.ds(pl.multiple_of(index * size, size), size)


def hbm(count):
    return [pl.BlockSpec(memory_space=pltpu.HBM)] * count


def hidden_kernel(layer, *refs):
    pieces, (gate_ref, up_ref, out_ref, gate_sum, up_sum) = refs[:-5], refs[-5:]
    gate_sum[...] = jnp.zeros_like(gate_sum)
    up_sum[...] = jnp.zeros_like(up_sum)
    start = 0
    for piece in pieces:

        @loop(piece.shape[1] // ROWS)
        def _(i):
            rows = piece[:, rows_at(i, ROWS)]
            at = pl.ds(pl.multiple_of(start + i * ROWS, ROWS), ROWS)
            gate_sum[...] += dot(rows, gate_ref[layer, 0, at, :])
            up_sum[...] += dot(rows, up_ref[layer, 0, at, :])

        start += piece.shape[1]
    out_ref[...] = silu_times(gate_sum[...], up_sum[...]).astype(out_ref.dtype)


def hidden_units(pieces, w_gate, w_up, layer):
    rows = pieces[0].shape[0]
    _, _, width, units = w_gate.shape
    return pl.pallas_call(
        functools.partial(hidden_kernel, layer),
        out_shape=jax.ShapeDtypeStruct((rows, units), BF16),
        in_specs=vmem(len(pieces) + 2),
        out_specs=vmem(1)[0],
        scratch_shapes=[pltpu.VMEM((rows, units), F32)] * 2,
        cost_estimate=pl.CostEstimate(
            flops=4 * rows * units * width, bytes_accessed=4 * units * width, transcendentals=rows * units
        ),
        compiler_params=pltpu.CompilerParams(vmem_limit_bytes=GRANT),
        name="hidden_units",
    )(*pieces, w_gate, w_up)


def down_kernel(*refs):
    count = len(STEPS)
    hidden, weights, out_ref = refs[:count], refs[count : 2 * count], refs[2 * count]

    @loop(out_ref.shape[0] // ROWS)
    def _(i):
        at = rows_at(i, ROWS)
        total = dot(hidden[0][at, :], weights[0][...])
        for hidden_ref, weight_ref in zip(hidden[1:], weights[1:]):
            total = total + dot(hidden_ref[at, :], weight_ref[...])
        out_ref[at, :] = total.astype(out_ref.dtype)


def down(hidden, weights):
    rows, units = hidden[0].shape
    part = weights[0].shape[1]
    return pl.pallas_call(
        down_kernel,
        out_shape=jax.ShapeDtypeStruct((rows, part), BF16),
        in_specs=vmem(2 * len(hidden)),
        out_specs=vmem(1)[0],
        cost_estimate=pl.CostEstimate(
            flops=2 * rows * units * part * len(hidden), bytes_accessed=2 * units * part * len(hidden), transcendentals=0
        ),
        compiler_params=pltpu.CompilerParams(vmem_limit_bytes=GRANT),
        name="down",
    )(*hidden, *weights)


def two_parts(value):
    high = value.astype(BF16)
    low = (value - high.astype(F32)).astype(BF16)
    lane = lax.broadcasted_iota(jnp.int32, (value.shape[0], LANES), 1)
    wide = jnp.where(lane == 0, high.astype(F32), jnp.where(lane == 1, low.astype(F32), 0.0))
    return wide.astype(BF16)


def one_value(parts):
    return jnp.sum(parts.astype(F32), axis=1, keepdims=True)


def spread_place(row, me, slots, capacity):
    n_dp = len(STEPS)
    place = row // slots
    away = jnp.where(place == 0, 0, jnp.where(place == 1, n_dp - 1, jnp.where(place == 2, 1, 2)))
    slot = row % slots
    return ((slot // capacity) * n_dp + (me + away) % n_dp) * capacity + slot % capacity


def partial_kernel(capacity, starts_ref, rows_ref, *refs):
    sources, (out_ref, arrived, sorted_ref, held, done) = refs[:-5], refs[-5:]
    count, _, units = held.shape
    total = sorted_ref.shape[0]
    first = pltpu.make_async_copy(rows_ref, arrived, done.at[count])
    copies = [pltpu.make_async_copy(source, held.at[k], done.at[k]) for k, source in enumerate(sources)]
    first.start()
    for copy in copies:
        copy.start()
    first.wait()

    @loop(total // ROWS)
    def _(i):
        at = rows_at(i, ROWS)
        row = lax.broadcasted_iota(jnp.int32, (ROWS, total), 0) + i * ROWS
        wanted = spread_place(row, starts_ref[count], total // len(STEPS), capacity)
        order = (wanted == lax.broadcasted_iota(jnp.int32, (ROWS, total), 1)).astype(F32).astype(BF16)
        rows = dot(order, arrived[...])
        sorted_ref[at, :] = rows.astype(BF16)
        out_ref[at, count * units :] = two_parts(jnp.sum(rows * rows, axis=1, keepdims=True))

    for copy in copies:
        copy.wait()

    @loop(count)
    def _(k):
        start = pl.multiple_of(starts_ref[k], units)
        out_ref[:, pl.ds(start, units)] = dot(sorted_ref[...], held[k]).astype(BF16)


def partial_products(me, rows, capacity, gates, ups):
    count, part = rows.shape
    n_dp = len(STEPS)
    units = gates[0].shape[1]
    weights = [weight for pair in zip(gates, ups) for weight in pair]
    starts = jnp.stack([(2 * ((me + step) % n_dp) + k) * units for step in STEPS for k in range(2)] + [me])
    return pl.pallas_call(
        functools.partial(partial_kernel, capacity),
        out_shape=jax.ShapeDtypeStruct((count, len(weights) * units + LANES), BF16),
        in_specs=[pl.BlockSpec(memory_space=pltpu.SMEM)] + hbm(1 + len(weights)),
        out_specs=vmem(1)[0],
        scratch_shapes=[
            pltpu.VMEM((count, part), BF16),
            pltpu.VMEM((count, part), BF16),
            pltpu.VMEM((len(weights), part, units), BF16),
            pltpu.SemaphoreType.DMA((len(weights) + 1,)),
        ],
        cost_estimate=pl.CostEstimate(
            flops=2 * count * part * (len(weights) * units + count), bytes_accessed=4 * n_dp * part * units, transcendentals=0
        ),
        compiler_params=pltpu.CompilerParams(vmem_limit_bytes=GRANT),
        name="partial_products",
    )(starts, rows, *weights)


def fold_kernel(left_ref, right_ref, from_left_ref, from_right_ref, left_out, right_out):
    half = from_left_ref.shape[0]
    last = left_ref.shape[1] - LANES
    for ref, arrived, out, at, other in (
        (right_ref, from_left_ref, right_out, slice(0, half), slice(half, 2 * half)),
        (left_ref, from_right_ref, left_out, slice(half, 2 * half), slice(0, half)),
    ):
        out[other, :] = ref[other, :]
        out[at, :last] = (ref[at, :last].astype(F32) + arrived[:, :last].astype(F32)).astype(BF16)
        out[at, last:] = two_parts(one_value(ref[at, last:]) + one_value(arrived[:, last:]))


def fold(products, from_left, from_right):
    height, width = products.shape[0] // len(STEPS), products.shape[1]
    return pl.pallas_call(
        fold_kernel,
        out_shape=[jax.ShapeDtypeStruct((height, width), BF16)] * 2,
        grid=(1,),
        in_specs=[pl.BlockSpec((height, width), lambda i: (1, 0)), pl.BlockSpec((height, width), lambda i: (2, 0))] + vmem(2),
        out_specs=vmem(2),
        cost_estimate=pl.CostEstimate(flops=height * width * 8, bytes_accessed=height * width * 8, transcendentals=0),
        compiler_params=pltpu.CompilerParams(vmem_limit_bytes=GRANT),
        name="fold",
    )(products, products, from_left, from_right)


def finish_kernel(layer, me_ref, products, left_ref, right_ref, w0, w1, w2, w3, w4, out_ref, hidden_ref, own_ref, held, done):
    n_dp = len(STEPS)
    units = w1.shape[0]
    half = units // 2
    width = out_ref.shape[1]
    last = own_ref.shape[1] - LANES
    first = pltpu.make_async_copy(products.at[: own_ref.shape[0]], own_ref, done.at[5])
    first.start()
    targets = [held.at[i] for i in range(3)] + [held.at[3, :half], held.at[3, half:]]
    copies = [
        pltpu.make_async_copy(source, target, done.at[k])
        for k, (source, target) in enumerate(zip((w0.at[layer, 0], w1, w2, w3, w4), targets))
    ]
    for copy in copies:
        copy.start()
    first.wait()

    def total(start, size):
        at = slice(start, start + size)
        return own_ref[:, at].astype(F32) + left_ref[:, at].astype(F32) + right_ref[:, at].astype(F32)

    square = one_value(own_ref[:, last:]) + one_value(left_ref[:, last:]) + one_value(right_ref[:, last:])
    scale = lax.rsqrt(square / width + EPS)
    for i in range(n_dp):
        gate = total(2 * i * units, units) * scale
        upper = total((2 * i + 1) * units, units) * scale
        hidden_ref[:, i * units : (i + 1) * units] = silu_times(gate, upper).astype(BF16)
    for copy in copies:
        copy.wait()

    def block(step):
        at = pl.multiple_of(((me_ref[0] + step + n_dp) % n_dp) * units, units)
        return hidden_ref[:, pl.ds(at, units)]

    @loop(width // CHUNK)
    def _(i):
        at = rows_at(i, CHUNK)
        result = dot(block(STEPS[0]), held[0, :, at])
        for k in range(1, n_dp):
            result = result + dot(block(STEPS[k]), held[k, :, at])
        out_ref[:, at] = result.astype(BF16)


def finish(me, products, left, right, w_down, layer, others):
    rows = left.shape[0]
    _, _, units, width = w_down.shape
    n_dp = len(STEPS)
    return pl.pallas_call(
        functools.partial(finish_kernel, layer),
        out_shape=jax.ShapeDtypeStruct((rows, width), BF16),
        in_specs=[pl.BlockSpec(memory_space=pltpu.SMEM)] + hbm(1) + vmem(2) + hbm(1 + len(others)),
        out_specs=vmem(1)[0],
        scratch_shapes=[
            pltpu.VMEM((rows, n_dp * units), BF16),
            pltpu.VMEM(left.shape, BF16),
            pltpu.VMEM((n_dp, units, width), BF16),
            pltpu.SemaphoreType.DMA((2 + len(others),)),
        ],
        cost_estimate=pl.CostEstimate(
            flops=2 * rows * n_dp * units * width, bytes_accessed=2 * n_dp * units * width, transcendentals=rows * n_dp * units
        ),
        compiler_params=pltpu.CompilerParams(vmem_limit_bytes=GRANT),
        name="finish",
    )(me, products, left, right, w_down, *others)


def slot_picks(ids, experts, capacity, lines):
    rows, top = ids.shape
    tokens = rows // lines
    expert_iota = lax.broadcasted_iota(jnp.int32, (lines, tokens * top, experts), 2)
    onehot = (ids.reshape(lines, tokens * top)[:, :, None] == expert_iota).astype(F32)
    before = jnp.tril(jnp.ones((tokens * top, tokens * top), F32), -1)
    earlier = jnp.einsum("ab,lbe->lae", before, onehot, preferred_element_type=F32)
    place = jnp.sum(earlier * onehot, axis=2).astype(jnp.int32).reshape(rows, top)
    line = lax.broadcasted_iota(jnp.int32, (rows, top), 0) // tokens
    target = (ids * lines + line) * capacity + place
    slot_iota = lax.broadcasted_iota(jnp.int32, (rows, top, experts * lines * capacity), 2)
    return target[:, :, None] == slot_iota


def gates_of(quant):
    wide = quant.astype(F32)
    return ROUTE_SCALE * wide / jnp.sum(wide, axis=1, keepdims=True)


def spread_of(picked, quant):
    return jnp.sum(jnp.where(picked, gates_of(quant)[:, :, None], 0.0), axis=1)


def chosen_of(picked):
    return jnp.any(picked, axis=1).astype(BF16)


def swap(rows):
    return lax.all_to_all(rows, EP, split_axis=0, concat_axis=0, tiled=True)


def weighted(spread, rows):
    return jnp.dot(spread, rows.astype(F32), precision=lax.Precision.HIGHEST, preferred_element_type=F32)


def per_device(tokens, expert_ids, quant_gates, w_gate, w_up, w_down):
    layers, count_tok, top = expert_ids.shape
    n_dp = lax.axis_size("dp")
    n_ep = lax.axis_size(EP)
    me = lax.axis_index("dp").astype(jnp.int32)
    me_vector = me.reshape(1)
    capacity = min(count_tok, max(2, 3 * count_tok * top // (2 * n_ep)))
    width = tokens.shape[1]
    units = w_gate.shape[3]
    part = width // n_dp
    slots = n_ep * capacity
    count = n_dp * slots

    def around(step, size):
        return ((me + step) % n_dp) * size

    wide = tokens.astype(F32)
    normed = (wide * lax.rsqrt(jnp.mean(wide * wide, axis=1, keepdims=True) + EPS)).astype(BF16)
    own_picks = [slot_picks(expert_ids[i], n_ep, capacity, 1) for i in range(layers)]
    arrived = swap(dot(chosen_of(own_picks[0]).T, normed).astype(BF16))

    down_slices = exchange(
        lambda step: lax.dynamic_slice(w_down, (0, 0, 0, around(step, part)), (1, 1, units, part))[0, 0]
    )
    routes = jnp.concatenate([*expert_ids, *quant_gates], axis=1).astype(BF16)
    routes = jnp.pad(routes, ((0, 0), (0, LANES - routes.shape[1])))
    line = exchange(
        lambda step: jnp.concatenate(
            [lax.dynamic_slice_in_dim(tokens, around(step, part), part, axis=1), routes], axis=1
        ),
    )
    line = place_blocks(line, 0)
    state = line[:, :part]
    routes = line[:, part:].astype(jnp.int32)
    line_ids = [routes[:, i * top : (i + 1) * top] for i in range(layers)]
    line_quant = [routes[:, (layers + i) * top : (layers + i + 1) * top] for i in range(layers)]
    line_picks = [slot_picks(ids, n_ep, capacity, n_dp) for ids in line_ids]
    expert_iota = lax.broadcasted_iota(jnp.int32, (1, 1, n_ep), 2)
    loads = jnp.stack([jnp.sum((ids[:, :, None] == expert_iota).astype(jnp.int32), axis=(0, 1)) for ids in line_ids])
    for axis in EP:
        loads = lax.psum(loads, axis)

    def rows_of(weight):
        return lambda step: lax.dynamic_slice(weight, (1, 0, around(step, part), 0), (1, 1, part, units))[0, 0]

    gates = exchange(rows_of(w_gate))
    ups = exchange(rows_of(w_up))
    whole_down = ring_gather(w_down[1, 0], 0)[1:]

    own, left, right, first, second = ring_gather(arrived, 1)
    hidden = []
    for block in (own, left, right):
        hidden.append(hidden_units([block], w_gate, w_up, 0))
    block = jnp.concatenate([first, second], axis=1)
    hidden.append(silu_times(dot(block, w_gate[0, 0]), dot(block, w_up[0, 0])).astype(BF16))
    hidden = jnp.concatenate(hidden, axis=0)
    out_row = lax.broadcasted_iota(jnp.int32, (count, count), 0)
    in_row = lax.broadcasted_iota(jnp.int32, (count, count), 1)
    moved = out_row == spread_place(in_row, me, slots, capacity)
    hidden = dot(moved.astype(BF16), hidden).astype(BF16)
    blocks = exchange(lambda step: hidden)
    returned = swap(down(blocks, down_slices))
    branch = weighted(spread_of(line_picks[0], line_quant[0]), returned)
    state = (state.astype(F32) + branch).astype(BF16)

    arrived = swap(dot(chosen_of(line_picks[1]).T, state).astype(BF16))
    own_rows = exchange(lambda step: lax.dynamic_slice_in_dim(state, around(step, count_tok), count_tok, axis=0))
    own_rows = place_blocks(own_rows, 1)
    products = partial_products(me, arrived, capacity, gates, ups)
    middle = count - slots // 2
    from_left, from_right = shift(products[count - slots : middle], 1), shift(products[middle:], -1)
    left, right = fold(products, from_left, from_right)
    from_left, from_right = shift(right, 1), shift(left, -1)
    message = finish(me_vector, products, from_left, from_right, w_down, 1, whole_down)
    returned = swap(message)
    branch = weighted(spread_of(own_picks[1], quant_gates[1]), returned)
    stream_out = (own_rows.astype(F32) + branch).astype(BF16)
    return (stream_out, loads)


def solution(mesh):
    finer = Mesh(mesh.devices.reshape(mesh.shape["dp"], 4, 8, 2), DP_EP)
    placed = (
        P(DP_EP, None),
        P(None, DP_EP, None),
        P(None, DP_EP, None),
        P(None, EP, None, "dp"),
        P(None, EP, None, "dp"),
        P(None, EP, "dp", None),
    )

    return jax.shard_map(per_device, mesh=finer, in_specs=placed, out_specs=(P(DP_EP, None), P()), check_vma=False)
```

```python
import functools

import jax
import jax.numpy as jnp
from jax import lax
from jax.experimental import pallas as pl
from jax.experimental.pallas import tpu as pltpu
from jax.sharding import Mesh
from jax.sharding import PartitionSpec as P


EP = ("ep_0", "ep_1", "ep_2")
DP_EP = ("dp", "ep_0", "ep_1", "ep_2")

ROUTE_SCALE = 2.827
EPS = 1e-06
BF16 = jnp.bfloat16
F32 = jnp.float32
LANES = 128
CHUNK = 512
ROWS = 256
GRANT = 20 * 1024 * 1024
STEPS = (0, -1, 1, 2)


def shift(array, step):
    n_dp = lax.axis_size("dp")
    return lax.ppermute(array, "dp", [(i, (i + step) % n_dp) for i in range(n_dp)])


def ring_gather(own, dim):
    half = own.shape[dim] // 2
    left, right = shift(own, 1), shift(own, -1)
    first = shift(lax.slice_in_dim(left, 0, half, axis=dim), 1)
    second = shift(lax.slice_in_dim(right, half, 2 * half, axis=dim), -1)
    return own, left, right, first, second


def exchange(piece_for):
    got = []
    for step in STEPS:
        got.append(shift(piece_for(-step), -step) if step else piece_for(0))
    return got


def place_blocks(blocks, dim):
    n_dp = lax.axis_size("dp")
    shape = list(blocks[0].shape)
    length = shape[dim]
    shape[dim] *= n_dp
    out = jnp.zeros(shape, blocks[0].dtype)
    for step, block in zip(STEPS, blocks):
        start = ((lax.axis_index("dp") + step) % n_dp) * length
        out = lax.dynamic_update_slice_in_dim(out, block, start, axis=dim)
    return out


def dot(a, b):
    return jnp.dot(a, b, preferred_element_type=F32)


def silu_times(gate, upper):
    return gate / (1.0 + jnp.exp(-gate)) * upper


def vmem(count):
    return [pl.BlockSpec(memory_space=pltpu.VMEM)] * count


def loop(count):
    return pl.loop(0, count)


def rows_at(index, size):
    return pl.ds(pl.multiple_of(index * size, size), size)


def hbm(count):
    return [pl.BlockSpec(memory_space=pltpu.HBM)] * count


def hidden_kernel(*refs):
    pieces, (gate_ref, up_ref, out_ref, gate_sum, up_sum) = refs[:-5], refs[-5:]
    gate_sum[...] = jnp.zeros_like(gate_sum)
    up_sum[...] = jnp.zeros_like(up_sum)
    start = 0
    for piece in pieces:

        @loop(piece.shape[1] // ROWS)
        def _(i):
            rows = piece[:, rows_at(i, ROWS)]
            at = pl.ds(pl.multiple_of(start + i * ROWS, ROWS), ROWS)
            gate_sum[...] += dot(rows, gate_ref[0, 0, at, :])
            up_sum[...] += dot(rows, up_ref[0, 0, at, :])

        start += piece.shape[1]
    out_ref[...] = silu_times(gate_sum[...], up_sum[...]).astype(out_ref.dtype)


def hidden_units(pieces, w_gate, w_up, layer):
    rows = pieces[0].shape[0]
    _, _, width, units = w_gate.shape
    return pl.pallas_call(
        hidden_kernel,
        out_shape=jax.ShapeDtypeStruct((rows, units), BF16),
        grid=(1,),
        in_specs=vmem(len(pieces)) + [pl.BlockSpec((1, 1, width, units), lambda i: (layer, 0, 0, 0))] * 2,
        out_specs=vmem(1)[0],
        scratch_shapes=[pltpu.VMEM((rows, units), F32)] * 2,
        cost_estimate=pl.CostEstimate(
            flops=4 * rows * units * width, bytes_accessed=4 * units * width, transcendentals=rows * units
        ),
        name="hidden_units",
    )(*pieces, w_gate, w_up)


def down_kernel(*refs):
    count = len(STEPS)
    hidden, weights, out_ref = refs[:count], refs[count : 2 * count], refs[2 * count]

    @loop(out_ref.shape[0] // ROWS)
    def _(i):
        at = rows_at(i, ROWS)
        total = dot(hidden[0][at, :], weights[0][...])
        for hidden_ref, weight_ref in zip(hidden[1:], weights[1:]):
            total = total + dot(hidden_ref[at, :], weight_ref[...])
        out_ref[at, :] = total.astype(out_ref.dtype)


def down(hidden, weights):
    rows, units = hidden[0].shape
    part = weights[0].shape[1]
    return pl.pallas_call(
        down_kernel,
        out_shape=jax.ShapeDtypeStruct((rows, part), BF16),
        in_specs=vmem(2 * len(hidden)),
        out_specs=vmem(1)[0],
        cost_estimate=pl.CostEstimate(
            flops=2 * rows * units * part * len(hidden), bytes_accessed=2 * units * part * len(hidden), transcendentals=0
        ),
        compiler_params=pltpu.CompilerParams(vmem_limit_bytes=GRANT),
        name="down",
    )(*hidden, *weights)


def two_parts(value):
    high = value.astype(BF16)
    low = (value - high.astype(F32)).astype(BF16)
    lane = lax.broadcasted_iota(jnp.int32, (value.shape[0], LANES), 1)
    wide = jnp.where(lane == 0, high.astype(F32), jnp.where(lane == 1, low.astype(F32), 0.0))
    return wide.astype(BF16)


def one_value(parts):
    return jnp.sum(parts.astype(F32), axis=1, keepdims=True)


def spread_place(row, me, slots, capacity):
    n_dp = len(STEPS)
    place = row // slots
    away = jnp.where(place == 0, 0, jnp.where(place == 1, n_dp - 1, jnp.where(place == 2, 1, 2)))
    slot = row % slots
    return ((slot // capacity) * n_dp + (me + away) % n_dp) * capacity + slot % capacity


def partial_kernel(capacity, starts_ref, rows_ref, *refs):
    sources, (out_ref, arrived, sorted_ref, held, done) = refs[:-5], refs[-5:]
    count, _, units = held.shape
    total = sorted_ref.shape[0]
    first = pltpu.make_async_copy(rows_ref, arrived, done.at[count])
    copies = [pltpu.make_async_copy(source, held.at[k], done.at[k]) for k, source in enumerate(sources)]
    first.start()
    for copy in copies:
        copy.start()
    first.wait()

    @loop(total // ROWS)
    def _(i):
        at = rows_at(i, ROWS)
        row = lax.broadcasted_iota(jnp.int32, (ROWS, total), 0) + i * ROWS
        wanted = spread_place(row, starts_ref[count], total // len(STEPS), capacity)
        order = (wanted == lax.broadcasted_iota(jnp.int32, (ROWS, total), 1)).astype(F32).astype(BF16)
        rows = dot(order, arrived[...])
        sorted_ref[at, :] = rows.astype(BF16)
        out_ref[at, count * units :] = two_parts(jnp.sum(rows * rows, axis=1, keepdims=True))

    for copy in copies:
        copy.wait()

    @loop(count)
    def _(k):
        start = pl.multiple_of(starts_ref[k], units)
        out_ref[:, pl.ds(start, units)] = dot(sorted_ref[...], held[k]).astype(BF16)


def partial_products(me, rows, capacity, gates, ups):
    count, part = rows.shape
    n_dp = len(STEPS)
    units = gates[0].shape[1]
    weights = [weight for pair in zip(gates, ups) for weight in pair]
    starts = jnp.stack([(2 * ((me + step) % n_dp) + k) * units for step in STEPS for k in range(2)] + [me])
    return pl.pallas_call(
        functools.partial(partial_kernel, capacity),
        out_shape=jax.ShapeDtypeStruct((count, len(weights) * units + LANES), BF16),
        in_specs=[pl.BlockSpec(memory_space=pltpu.SMEM)] + hbm(1 + len(weights)),
        out_specs=vmem(1)[0],
        scratch_shapes=[
            pltpu.VMEM((count, part), BF16),
            pltpu.VMEM((count, part), BF16),
            pltpu.VMEM((len(weights), part, units), BF16),
            pltpu.SemaphoreType.DMA((len(weights) + 1,)),
        ],
        cost_estimate=pl.CostEstimate(
            flops=2 * count * part * (len(weights) * units + count), bytes_accessed=4 * n_dp * part * units, transcendentals=0
        ),
        compiler_params=pltpu.CompilerParams(vmem_limit_bytes=GRANT),
        name="partial_products",
    )(starts, rows, *weights)


def fold_kernel(left_ref, right_ref, from_left_ref, from_right_ref, left_out, right_out):
    half = from_left_ref.shape[0]
    last = left_ref.shape[1] - LANES
    for ref, arrived, out, at, other in (
        (right_ref, from_left_ref, right_out, slice(0, half), slice(half, 2 * half)),
        (left_ref, from_right_ref, left_out, slice(half, 2 * half), slice(0, half)),
    ):
        out[other, :] = ref[other, :]
        out[at, :last] = (ref[at, :last].astype(F32) + arrived[:, :last].astype(F32)).astype(BF16)
        out[at, last:] = two_parts(one_value(ref[at, last:]) + one_value(arrived[:, last:]))


def fold(products, from_left, from_right):
    height, width = products.shape[0] // len(STEPS), products.shape[1]
    return pl.pallas_call(
        fold_kernel,
        out_shape=[jax.ShapeDtypeStruct((height, width), BF16)] * 2,
        grid=(1,),
        in_specs=[pl.BlockSpec((height, width), lambda i: (1, 0)), pl.BlockSpec((height, width), lambda i: (2, 0))] + vmem(2),
        out_specs=vmem(2),
        cost_estimate=pl.CostEstimate(flops=height * width * 8, bytes_accessed=height * width * 8, transcendentals=0),
        compiler_params=pltpu.CompilerParams(vmem_limit_bytes=GRANT),
        name="fold",
    )(products, products, from_left, from_right)


def finish_kernel(layer, me_ref, products, left_ref, right_ref, w0, w1, w2, w3, w4, out_ref, hidden_ref, own_ref, held, done):
    n_dp = len(STEPS)
    units = w1.shape[0]
    half = units // 2
    width = out_ref.shape[1]
    last = own_ref.shape[1] - LANES
    first = pltpu.make_async_copy(products.at[: own_ref.shape[0]], own_ref, done.at[5])
    first.start()
    targets = [held.at[i] for i in range(3)] + [held.at[3, :half], held.at[3, half:]]
    copies = [
        pltpu.make_async_copy(source, target, done.at[k])
        for k, (source, target) in enumerate(zip((w0.at[layer, 0], w1, w2, w3, w4), targets))
    ]
    for copy in copies:
        copy.start()
    first.wait()

    def total(start, size):
        at = slice(start, start + size)
        return own_ref[:, at].astype(F32) + left_ref[:, at].astype(F32) + right_ref[:, at].astype(F32)

    square = one_value(own_ref[:, last:]) + one_value(left_ref[:, last:]) + one_value(right_ref[:, last:])
    scale = lax.rsqrt(square / width + EPS)
    for i in range(n_dp):
        gate = total(2 * i * units, units) * scale
        upper = total((2 * i + 1) * units, units) * scale
        hidden_ref[:, i * units : (i + 1) * units] = silu_times(gate, upper).astype(BF16)
    for copy in copies:
        copy.wait()

    def block(step):
        at = pl.multiple_of(((me_ref[0] + step + n_dp) % n_dp) * units, units)
        return hidden_ref[:, pl.ds(at, units)]

    @loop(width // CHUNK)
    def _(i):
        at = rows_at(i, CHUNK)
        result = dot(block(STEPS[0]), held[0, :, at])
        for k in range(1, n_dp):
            result = result + dot(block(STEPS[k]), held[k, :, at])
        out_ref[:, at] = result.astype(BF16)


def finish(me, products, left, right, w_down, layer, others):
    rows = left.shape[0]
    _, _, units, width = w_down.shape
    n_dp = len(STEPS)
    return pl.pallas_call(
        functools.partial(finish_kernel, layer),
        out_shape=jax.ShapeDtypeStruct((rows, width), BF16),
        in_specs=[pl.BlockSpec(memory_space=pltpu.SMEM)] + hbm(1) + vmem(2) + hbm(1 + len(others)),
        out_specs=vmem(1)[0],
        scratch_shapes=[
            pltpu.VMEM((rows, n_dp * units), BF16),
            pltpu.VMEM(left.shape, BF16),
            pltpu.VMEM((n_dp, units, width), BF16),
            pltpu.SemaphoreType.DMA((2 + len(others),)),
        ],
        cost_estimate=pl.CostEstimate(
            flops=2 * rows * n_dp * units * width, bytes_accessed=2 * n_dp * units * width, transcendentals=rows * n_dp * units
        ),
        compiler_params=pltpu.CompilerParams(vmem_limit_bytes=GRANT),
        name="finish",
    )(me, products, left, right, w_down, *others)


def slot_picks(ids, experts, capacity, lines):
    rows, top = ids.shape
    tokens = rows // lines
    expert_iota = lax.broadcasted_iota(jnp.int32, (lines, tokens * top, experts), 2)
    onehot = (ids.reshape(lines, tokens * top)[:, :, None] == expert_iota).astype(F32)
    before = jnp.tril(jnp.ones((tokens * top, tokens * top), F32), -1)
    earlier = jnp.einsum("ab,lbe->lae", before, onehot, preferred_element_type=F32)
    place = jnp.sum(earlier * onehot, axis=2).astype(jnp.int32).reshape(rows, top)
    line = lax.broadcasted_iota(jnp.int32, (rows, top), 0) // tokens
    target = (ids * lines + line) * capacity + place
    slot_iota = lax.broadcasted_iota(jnp.int32, (rows, top, experts * lines * capacity), 2)
    return target[:, :, None] == slot_iota


def gates_of(quant):
    wide = quant.astype(F32)
    return ROUTE_SCALE * wide / jnp.sum(wide, axis=1, keepdims=True)


def spread_of(picked, quant):
    return jnp.sum(jnp.where(picked, gates_of(quant)[:, :, None], 0.0), axis=1)


def chosen_of(picked):
    return jnp.any(picked, axis=1).astype(BF16)


def swap(rows):
    return lax.all_to_all(rows, EP, split_axis=0, concat_axis=0, tiled=True)


def weighted(spread, rows):
    return jnp.dot(spread, rows.astype(F32), precision=lax.Precision.HIGHEST, preferred_element_type=F32)


def per_device(tokens, expert_ids, quant_gates, w_gate, w_up, w_down):
    layers, count_tok, top = expert_ids.shape
    n_dp = lax.axis_size("dp")
    n_ep = lax.axis_size(EP)
    me = lax.axis_index("dp").astype(jnp.int32)
    me_vector = me.reshape(1)
    capacity = min(count_tok, max(2, 3 * count_tok * top // (2 * n_ep)))
    width = tokens.shape[1]
    units = w_gate.shape[3]
    part = width // n_dp
    slots = n_ep * capacity
    count = n_dp * slots

    def around(step, size):
        return ((me + step) % n_dp) * size

    wide = tokens.astype(F32)
    normed = (wide * lax.rsqrt(jnp.mean(wide * wide, axis=1, keepdims=True) + EPS)).astype(BF16)
    own_picks = [slot_picks(expert_ids[i], n_ep, capacity, 1) for i in range(layers)]
    arrived = swap(dot(chosen_of(own_picks[0]).T, normed).astype(BF16))

    down_slices = exchange(
        lambda step: lax.dynamic_slice(w_down, (0, 0, 0, around(step, part)), (1, 1, units, part))[0, 0]
    )
    routes = jnp.concatenate([*expert_ids, *quant_gates], axis=1).astype(BF16)
    routes = jnp.pad(routes, ((0, 0), (0, LANES - routes.shape[1])))
    line = exchange(
        lambda step: jnp.concatenate(
            [lax.dynamic_slice_in_dim(tokens, around(step, part), part, axis=1), routes], axis=1
        ),
    )
    line = place_blocks(line, 0)
    state = line[:, :part]
    routes = line[:, part:].astype(jnp.int32)
    line_ids = [routes[:, i * top : (i + 1) * top] for i in range(layers)]
    line_quant = [routes[:, (layers + i) * top : (layers + i + 1) * top] for i in range(layers)]
    line_picks = [slot_picks(ids, n_ep, capacity, n_dp) for ids in line_ids]
    expert_iota = lax.broadcasted_iota(jnp.int32, (1, 1, n_ep), 2)
    loads = jnp.stack([jnp.sum((ids[:, :, None] == expert_iota).astype(jnp.int32), axis=(0, 1)) for ids in line_ids])
    for axis in EP:
        loads = lax.psum(loads, axis)

    def rows_of(weight):
        return lambda step: lax.dynamic_slice(weight, (1, 0, around(step, part), 0), (1, 1, part, units))[0, 0]

    gates = exchange(rows_of(w_gate))
    ups = exchange(rows_of(w_up))
    whole_down = ring_gather(w_down[1, 0], 0)[1:]

    own, left, right, first, second = ring_gather(arrived, 1)
    hidden = []
    for block in (own, left, right):
        hidden.append(hidden_units([block], w_gate, w_up, 0))
    block = jnp.concatenate([first, second], axis=1)
    hidden.append(silu_times(dot(block, w_gate[0, 0]), dot(block, w_up[0, 0])).astype(BF16))
    hidden = jnp.concatenate(hidden, axis=0)
    out_row = lax.broadcasted_iota(jnp.int32, (count, count), 0)
    in_row = lax.broadcasted_iota(jnp.int32, (count, count), 1)
    moved = out_row == spread_place(in_row, me, slots, capacity)
    hidden = dot(moved.astype(BF16), hidden).astype(BF16)
    blocks = exchange(lambda step: hidden)
    returned = swap(down(blocks, down_slices))
    branch = weighted(spread_of(line_picks[0], line_quant[0]), returned)
    state = (state.astype(F32) + branch).astype(BF16)

    arrived = swap(dot(chosen_of(line_picks[1]).T, state).astype(BF16))
    own_rows = exchange(lambda step: lax.dynamic_slice_in_dim(state, around(step, count_tok), count_tok, axis=0))
    own_rows = place_blocks(own_rows, 1)
    products = partial_products(me, arrived, capacity, gates, ups)
    middle = count - slots // 2
    from_left, from_right = shift(products[count - slots : middle], 1), shift(products[middle:], -1)
    left, right = fold(products, from_left, from_right)
    from_left, from_right = shift(right, 1), shift(left, -1)
    message = finish(me_vector, products, from_left, from_right, w_down, 1, whole_down)
    returned = swap(message)
    branch = weighted(spread_of(own_picks[1], quant_gates[1]), returned)
    stream_out = (own_rows.astype(F32) + branch).astype(BF16)
    return (stream_out, loads)


def solution(mesh):
    finer = Mesh(mesh.devices.reshape(mesh.shape["dp"], 4, 8, 2), DP_EP)
    placed = (
        P(DP_EP, None),
        P(None, DP_EP, None),
        P(None, DP_EP, None),
        P(None, EP, None, "dp"),
        P(None, EP, None, "dp"),
        P(None, EP, "dp", None),
    )

    return jax.shard_map(per_device, mesh=finer, in_specs=placed, out_specs=(P(DP_EP, None), P()), check_vma=False)
```
